128 devices in a mesh: dp: 1, sp: 128 (over z, y, x, core).
Axes of the slice: x: 4, y: 4, z: 4, core: 2. Of those that a mesh axis runs over, the one named last changes fastest.
Arguments:
- z_points: bfloat16 [262144, 384], P(('dp', 'sp'))
- x_points: bfloat16 [16384, 384], P(('dp', 'sp'))
- rhs_vals: bfloat16 [16384, 64], P(('dp', 'sp'))
- block_mask: int32 [128, 128], P(('dp', 'sp'))
- length_scale: float32 [1], replicated
- out_scale: float32 [1], replicated
Outputs:
- output: float32 [262144, 64], P(('dp', 'sp'))
All inputs are finite; a program needn't handle non-finite values.
Results may differ from the reference program's by a relative error of at most 0.001.
Values are sent between devices in bfloat16 or wider.
A program may use at most 1 GiB of HBM per device.

```python
import jax
import jax.numpy as jnp
from jax import lax

D = 384
R = 64
SP = 128
TGT_DEV = 2048
SRC_DEV = 128
CLUSTERS = 8
M_TGT = SP * TGT_DEV
N_SRC = SP * SRC_DEV


def draw_mask(mask_key):
    key_a, key_b = jax.random.split(mask_key)
    mask_draws = jax.random.randint(key_a, (SP, SP), 0, SP)
    limits = jax.random.randint(key_b, (SP, 1), 1, SP + 1)
    on_diag = jnp.arange(SP)[:, None] == jnp.arange(SP)[None, :]
    return jnp.where((mask_draws < limits) | on_diag, 1, 0).astype(jnp.int32)


def setup_inputs(seed: int = 0, part: int = 0) -> dict:
    base_key = jax.random.key(seed)
    shared_key, part_base = jax.random.split(base_key)
    part_key = jax.random.fold_in(part_base, part)
    key_list = jax.random.split(part_key, 9)
    centers = jax.random.normal(key_list[0], (CLUSTERS, D), jnp.float32)
    z_labels = jax.random.randint(key_list[1], (M_TGT,), 0, CLUSTERS)
    x_labels = jax.random.randint(key_list[2], (N_SRC,), 0, CLUSTERS)
    z_vals = centers[z_labels] + 0.5 * jax.random.normal(key_list[3], (M_TGT, D), jnp.float32)
    x_vals = centers[x_labels] + 0.5 * jax.random.normal(key_list[4], (N_SRC, D), jnp.float32)
    col_mean = jax.random.uniform(key_list[5], (1, R), jnp.float32, minval=0.5, maxval=1.5)
    cluster_offs = jax.random.normal(key_list[6], (CLUSTERS, R), jnp.float32)
    rhs_noise = jax.random.normal(key_list[7], (N_SRC, R), jnp.float32)
    rhs = (col_mean + cluster_offs[x_labels] + rhs_noise) * (4.0 / N_SRC)
    block_mask = draw_mask(key_list[8])
    scale_keys = jax.random.split(shared_key)
    length_scale = jnp.sqrt(D * jax.random.uniform(scale_keys[0], (1,), jnp.float32, minval=0.8, maxval=1.4))
    out_scale = jax.random.uniform(scale_keys[1], (1,), jnp.float32, minval=0.5, maxval=1.5)
    return {
        "z_points": z_vals.astype(jnp.bfloat16),
        "x_points": x_vals.astype(jnp.bfloat16),
        "rhs_vals": rhs.astype(jnp.bfloat16),
        "block_mask": block_mask,
        "length_scale": length_scale,
        "out_scale": out_scale,
    }


def reference(z_points, x_points, rhs_vals, block_mask, length_scale, out_scale):
    ell_sq = length_scale[0] * length_scale[0]
    x_f32 = x_points.astype(jnp.float32)
    x_norm = jnp.sum(x_f32 * x_f32, axis=1)
    v_blocks = rhs_vals.reshape(SP, SRC_DEV, R)
    z_blocks = z_points.reshape(SP, TGT_DEV, D)

    def one_block(block_in):
        z_rows, mask_row = block_in
        z_f32 = z_rows.astype(jnp.float32)
        z_norm = jnp.sum(z_f32 * z_f32, axis=1)
        gram_mat = jnp.dot(z_rows, x_points.T, preferred_element_type=jnp.float32)
        sq_dist = jnp.maximum(z_norm[:, None] + x_norm[None, :] - 2.0 * gram_mat, 0.0)
        kern_mat = (out_scale[0] * jnp.exp(-sq_dist / (2.0 * ell_sq))).astype(jnp.bfloat16)
        v_masked = (v_blocks * mask_row[:, None, None].astype(jnp.bfloat16)).reshape(N_SRC, R)
        return jnp.dot(kern_mat, v_masked, preferred_element_type=jnp.float32)

    y_blocks = lax.map(one_block, (z_blocks, block_mask))
    return y_blocks.reshape(M_TGT, R)
```

```python
import functools

import jax
import jax.numpy as jnp
from jax import lax
from jax.experimental import pallas as pl
from jax.experimental.pallas import tpu as pltpu
from jax.sharding import PartitionSpec as P

MESH = pl.DeviceIdType.MESH
F32 = jnp.float32
BF16 = jnp.bfloat16
LOG2E = 1.4426950408889634
ROWS = 128
PIECES = ((0, 48), (48, 48), (96, 32))
GROUP = 4
TILES = 4
EARLY = 2


def item_order(ring):
    hops = [(i, j, k) for i in range(ring) for j in range(ring) for k in range(ring)]
    return sorted(hops, key=lambda h: (sum(h), h[2], h[1], h[0]))


def split3(val):
    hi = val.astype(BF16).astype(F32)
    rest = val - hi
    mid = rest.astype(BF16).astype(F32)
    return hi, mid, (rest - mid).astype(BF16).astype(F32)


def kernel(ring, x_hbm, z_hbm, w_ref, ell_ref, scale_ref, y_ref,
           xb, zv, zt, aug, vt, ks, wsm, in_sem, recv_sem, pair_sem, send_sem):
    order = item_order(ring)
    slot_of = {h: n for n, h in enumerate(order)}
    n_items = len(order)
    n_groups = n_items // GROUP
    half = GROUP * ROWS
    tile = zv.shape[0] // TILES

    me = lax.axis_index("sp")
    core = me % 2
    pos = [(me // 2) % ring, (me // (2 * ring)) % ring, me // (2 * ring * ring)]
    step = 1 - 2 * core
    shifted = [[(p + (ring - h) * step + ring * ring) % ring for h in range(ring)] for p in pos]

    def device(x, y, z, c):
        return ((z * ring + y) * ring + x) * 2 + c

    downstream, upstream = [], []
    for axis in range(3):
        for lst, hop in ((downstream, ring - 1), (upstream, 1)):
            at = [shifted[a][hop] if a == axis else pos[a] for a in range(3)]
            lst.append(device(*at, core))
    partner = me + step

    own_in = pltpu.make_async_copy(x_hbm, xb.at[0], in_sem.at[0])
    z_in = pltpu.make_async_copy(z_hbm, zv, in_sem.at[1])
    own_in.start()
    z_in.start()
    barrier = pltpu.get_barrier_semaphore()
    for other in (*downstream, *upstream, partner):
        pl.semaphore_signal(barrier, inc=1, device_id={"sp": other}, device_id_type=MESH)
    pl.semaphore_wait(barrier, 7)
    own_in.wait()

    def slot_index(n):
        return (n // GROUP) * 2 * GROUP + n % GROUP

    sent = [0] * n_groups

    def forward(n):
        i, j, k = order[n]
        src = slot_index(n)
        for leg in range(3):
            if leg == 0:
                child = (i + 1, j, k) if j == 0 and k == 0 else None
            elif leg == 1:
                child = (i, j + 1, k) if k == 0 else None
            else:
                child = (i, j, k + 1)
            if child is None or child not in slot_of:
                continue
            m = slot_of[child]
            for colour, (lo, cnt) in enumerate(PIECES):
                pltpu.make_async_remote_copy(
                    src_ref=xb.at[src, pl.ds(lo, cnt)],
                    dst_ref=xb.at[slot_index(m), pl.ds(lo, cnt)],
                    send_sem=send_sem.at[n // GROUP],
                    recv_sem=recv_sem.at[m],
                    device_id={"sp": downstream[(colour + leg) % 3]},
                    device_id_type=MESH,
                ).start()
            sent[n // GROUP] += 1

    def arrive(n):
        dst = xb.at[slot_index(n)]
        pltpu.make_async_copy(dst, dst, recv_sem.at[n]).wait()

    def to_partner(q):
        pltpu.make_async_remote_copy(
            src_ref=xb.at[pl.ds(2 * GROUP * q, GROUP)],
            dst_ref=xb.at[pl.ds(2 * GROUP * (q + 1) + GROUP, GROUP)],
            send_sem=send_sem.at[q],
            recv_sem=pair_sem.at[q],
            device_id={"sp": partner},
            device_id_type=MESH,
        ).start()
        sent[q] += GROUP

    def from_partner(q):
        dst = xb.at[pl.ds(2 * GROUP * (q + 1) + GROUP, GROUP)]
        pltpu.make_async_copy(dst, dst, pair_sem.at[q]).wait()

    def mask_words(n, theirs):
        slot = slot_index(n) + (3 * GROUP if theirs else 0)
        for colour in range(3):
            at = [None] * 3
            for leg in range(3):
                axis = (colour + leg) % 3
                hop = order[n][leg]
                at[axis] = shifted[axis][(ring - hop) % ring if theirs else hop]
            wsm[slot * 3 + colour] = w_ref[0, device(*at, 1 - core if theirs else core)]

    lane = lax.broadcasted_iota(jnp.int32, (1, 128), 1)
    lane_full = lax.broadcasted_iota(jnp.int32, (ROWS, 128), 1)

    def prepare(slot, buf, place):
        x = xb[slot, :, 0:384].astype(F32)
        sq = x * x
        nx = jnp.sum(sq[:, 0:128] + sq[:, 128:256] + sq[:, 256:384], axis=1, keepdims=True)
        hi, mid, low = split3(-0.5 * nx)
        cols = jnp.where(lane_full < 3, 1.0, 0.0)
        cols = jnp.where(lane_full == 3, hi, cols)
        cols = jnp.where(lane_full == 4, mid, cols)
        cols = jnp.where(lane_full == 5, low, cols)
        base = pl.multiple_of(place * ROWS, ROWS)
        aug[buf, pl.ds(base, ROWS), :] = cols.astype(BF16)
        w = jnp.where(lane < 48, wsm[slot * 3], jnp.where(lane < 96, wsm[slot * 3 + 1], wsm[slot * 3 + 2]))
        v_t = xb[slot, :, 384:512].T[0:64, :]
        vt[buf, :, pl.ds(base, ROWS)] = (v_t.astype(F32) * w.astype(F32)).astype(BF16)

    forward(0)
    for n in range(GROUP):
        mask_words(n, False)

    vt[...] = jnp.zeros_like(vt)
    ks[...] = jnp.zeros_like(ks)
    y_ref[...] = jnp.zeros_like(y_ref)
    z_in.wait()
    row = lax.broadcasted_iota(jnp.int32, (128, tile), 0)

    def prepare_targets(r, carry):
        base = pl.multiple_of(r * tile, tile)
        zr = zv[pl.ds(base, tile), :].T
        zt[0:384, pl.ds(base, tile)] = zr
        zf = zr.astype(F32)
        hi, mid, low = split3(-0.5 * jnp.sum(zf * zf, axis=0, keepdims=True))
        rows = jnp.where(row == 0, hi, jnp.where(row == 1, mid, jnp.where(row == 2, low, 0.0)))
        rows = jnp.where((row >= 3) & (row < 6), 1.0, rows)
        zt[384:512, pl.ds(base, tile)] = rows.astype(BF16)
        return carry

    lax.fori_loop(0, TILES, prepare_targets, 0)
    ell = jnp.full((1, tile), ell_ref[0], F32)
    rate = LOG2E / (ell * ell)
    scale = scale_ref[0]

    prepare(0, 0, 0)
    for n in range(1, GROUP):
        arrive(n)
        forward(n)
    to_partner(0)
    for n in range(1, GROUP):
        prepare(slot_index(n), 0, n)

    def product(buf, prev, at):
        base = pl.multiple_of(at * tile, tile)
        y_ref[:, pl.ds(base, tile)] += jnp.dot(vt[buf], ks[prev], preferred_element_type=F32)

    def run_chunk(g, prep):
        first = 2 * GROUP * g + (GROUP if g == n_groups else 0)
        count = GROUP if g in (0, n_groups) else 2 * GROUP
        rows = count * ROWS

        def body(r, carry):
            now = r % 2
            src = xb[pl.ds(first, count)].reshape(rows, 512)[:, 0:384]
            lhs = jnp.concatenate([src, aug[g % 3, 0:rows, :]], axis=1)
            base = pl.multiple_of(r * tile, tile)
            neg = jnp.dot(lhs, zt[:, pl.ds(base, tile)], preferred_element_type=F32)
            val = jnp.exp2(jnp.minimum(neg * rate, 0.0)) * scale
            ks[now, 0:rows, :] = val.astype(BF16)
            buf = jnp.where(r == 0, (g + 2) % 3, g % 3)
            product(buf, 1 - now, (r + TILES - 1) % TILES)
            if prep:
                prepare_next(g + 1, r)
            return carry

        lax.fori_loop(0, TILES, body, 0)

    def prepare_next(n, r):
        if n < n_groups:
            prepare(2 * GROUP * n + r, n % 3, r)
        if n >= 1:
            prepare(2 * GROUP * n + GROUP + r, n % 3, r + (0 if n == n_groups else GROUP))

    def communicate(n):
        if n < n_groups:
            for m in range(GROUP * n, GROUP * (n + 1)):
                mask_words(m, False)
                arrive(m)
                forward(m)
            to_partner(n)
        for m in range(GROUP * (n - 1), GROUP * n):
            mask_words(m, True)
        from_partner(n - 1)
        if n == n_groups:
            vt[n % 3, :, half:] = jnp.zeros((64, half), BF16)

    for g in range(n_groups + 1):
        if g == n_groups:
            run_chunk(g, False)
        elif g < EARLY:
            run_chunk(g, False)
            communicate(g + 1)

            def prep_body(r, carry, n=g + 1):
                prepare_next(n, r)
                return carry

            lax.fori_loop(0, GROUP, prep_body, 0)
        else:
            communicate(g + 1)
            run_chunk(g, True)
    product(n_groups % 3, (TILES - 1) % 2, TILES - 1)
    for q in range(n_groups):
        done = xb.at[pl.ds(0, sent[q])]
        pltpu.make_async_copy(done, done, send_sem.at[q]).wait()


def solution(mesh):
    devices = mesh.shape["sp"]
    ring = round((devices // 2) ** (1 / 3))
    n_items = ring**3
    n_groups = n_items // GROUP
    row_spec = P(("dp", "sp"), None)

    def local_fn(z_rows, x_rows, v_rows, mask_row, length_scale, out_scale):
        targets = z_rows.shape[0]
        tile = targets // TILES
        pad = jnp.zeros((ROWS, 128 - v_rows.shape[1]), BF16)
        packed = jnp.concatenate([x_rows, v_rows, pad], axis=1)
        y_t = pl.pallas_call(
            functools.partial(kernel, ring),
            out_shape=jax.ShapeDtypeStruct((64, targets), F32),
            in_specs=[
                pl.BlockSpec(memory_space=pl.ANY),
                pl.BlockSpec(memory_space=pl.ANY),
                pl.BlockSpec(memory_space=pltpu.SMEM),
                pl.BlockSpec(memory_space=pltpu.SMEM),
                pl.BlockSpec(memory_space=pltpu.SMEM),
            ],
            out_specs=pl.BlockSpec(memory_space=pltpu.VMEM),
            scratch_shapes=[
                pltpu.VMEM((2 * GROUP * (n_groups + 1), ROWS, 512), BF16),
                pltpu.VMEM((targets, 384), BF16),
                pltpu.VMEM((512, targets), BF16),
                pltpu.VMEM((3, 2 * GROUP * ROWS, 128), BF16),
                pltpu.VMEM((3, 64, 2 * GROUP * ROWS), BF16),
                pltpu.VMEM((2, 2 * GROUP * ROWS, tile), BF16),
                pltpu.SMEM((2 * GROUP * (n_groups + 1) * 3,), jnp.int32),
                pltpu.SemaphoreType.DMA((2,)),
                pltpu.SemaphoreType.DMA((n_items,)),
                pltpu.SemaphoreType.DMA((n_groups,)),
                pltpu.SemaphoreType.DMA((n_groups,)),
            ],
            compiler_params=pltpu.CompilerParams(
                collective_id=0, has_side_effects=True, vmem_limit_bytes=60 * 2**20
            ),
            name="gather_product",
        )(packed, z_rows, mask_row, length_scale, out_scale)
        return y_t.T

    return jax.shard_map(
        local_fn,
        mesh=mesh,
        in_specs=(row_spec, row_spec, row_spec, row_spec, P(None), P(None)),
        out_specs=row_spec,
        check_vma=False,
    )
```

```python
import functools

import jax
import jax.numpy as jnp
from jax import lax
from jax.experimental import pallas as pl
from jax.experimental.pallas import tpu as pltpu
from jax.sharding import PartitionSpec as P

MESH = pl.DeviceIdType.MESH
F32 = jnp.float32
BF16 = jnp.bfloat16
LOG2E = 1.4426950408889634
ROWS = 128
PIECES = ((0, 32, 0, 1), (32, 16, 0, -1), (48, 32, 1, 1), (80, 16, 1, -1), (96, 16, 2, 1), (112, 16, 2, -1))
TILES = 4
EARLY = 1


def line_order(ring):
    hops = [(j, k) for j in range(ring) for k in range(ring)]
    return sorted(hops, key=lambda h: (sum(h), h[1], h[0]))


def split3(val):
    hi = val.astype(BF16).astype(F32)
    rest = val - hi
    mid = rest.astype(BF16).astype(F32)
    return hi, mid, (rest - mid).astype(BF16).astype(F32)


def kernel(ring, x_hbm, z_hbm, w_ref, ell_ref, scale_ref, y_ref,
           xb, zv, zt, aug0, aug1, stage, vt, ks0, ks1, wsm, in_sem, recv_sem, pair_sem, send_sem):
    order = line_order(ring)
    slot_of = {h: n for n, h in enumerate(order)}
    n_groups = len(order)
    half = ring * ROWS
    tile = zv.shape[0] // TILES
    aug = (aug0, aug1)
    per_body = ring // (TILES // 2)

    me = lax.axis_index("sp")
    core = me % 2
    pos = [(me // 2) % ring, (me // (2 * ring)) % ring, me // (2 * ring * ring)]
    step = 1 - 2 * core
    shifted = [[(p + (ring - h) * step + ring * ring) % ring for h in range(ring)] for p in pos]

    def device(coords, c):
        x, y, z = coords
        return ((z * ring + y) * ring + x) * 2 + c

    def upstream(axis, sign, hop):
        return shifted[axis][hop if sign > 0 else (ring - hop) % ring]

    def downstream(axis, sign, hop):
        at = list(pos)
        at[axis] = upstream(axis, sign, (ring - hop) % ring)
        return device(at, core)

    partner = me + step

    own_in = pltpu.make_async_copy(x_hbm, xb.at[0], in_sem.at[0])
    z_in = pltpu.make_async_copy(z_hbm, zv, in_sem.at[1])
    own_in.start()
    z_in.start()
    barrier = pltpu.get_barrier_semaphore()
    others = [downstream(axis, 1, hop) for axis in range(3) for hop in range(1, ring)] + [partner]
    for other in others:
        pl.semaphore_signal(barrier, inc=1, device_id={"sp": other}, device_id_type=MESH)
    pl.semaphore_wait(barrier, len(others))
    own_in.wait()

    sent = [0] * n_groups

    def send(src, dst, axis, sign, hop, q, m):
        pltpu.make_async_remote_copy(
            src_ref=src,
            dst_ref=dst,
            send_sem=send_sem.at[q],
            recv_sem=recv_sem.at[m],
            device_id={"sp": downstream(axis, sign, hop)},
            device_id_type=MESH,
        ).start()

    def send_own():
        for hop in sorted(range(1, ring), key=lambda h: min(h, ring - h)):
            for lo, cnt, rot, sign in PIECES:
                rows = pl.ds(lo, cnt)
                send(xb.at[0, rows], xb.at[hop, rows], rot, sign, hop, 0, 0)
            sent[0] += 1

    def forward(q):
        j, k = order[q]
        for leg, child in ((1, (j + 1, k) if k == 0 else None), (2, (j, k + 1))):
            if child not in slot_of:
                continue
            m = slot_of[child]
            for lo, cnt, rot, sign in PIECES:
                rows = pl.ds(lo, cnt)
                send(
                    xb.at[pl.ds(2 * ring * q, ring), rows],
                    xb.at[pl.ds(2 * ring * m, ring), rows],
                    (rot + leg) % 3, sign, 1, q, m,
                )
            sent[q] += ring

    def arrive(q):
        dst = xb.at[pl.ds(1, ring - 1)] if q == 0 else xb.at[pl.ds(2 * ring * q, ring)]
        pltpu.make_async_copy(dst, dst, recv_sem.at[q]).wait()

    def to_partner(q):
        pltpu.make_async_remote_copy(
            src_ref=xb.at[pl.ds(2 * ring * q, ring)],
            dst_ref=xb.at[pl.ds(2 * ring * (q + 1) + ring, ring)],
            send_sem=send_sem.at[q],
            recv_sem=pair_sem.at[q],
            device_id={"sp": partner},
            device_id_type=MESH,
        ).start()
        sent[q] += ring

    def from_partner(q):
        dst = xb.at[pl.ds(2 * ring * (q + 1) + ring, ring)]
        pltpu.make_async_copy(dst, dst, pair_sem.at[q]).wait()

    def mask_words(q, theirs):
        for i in range(ring):
            slot = (2 * ring * (q + 1) + ring if theirs else 2 * ring * q) + i
            for p, (_, _, rot, sign) in enumerate(PIECES):
                at = [None] * 3
                for leg, hop in enumerate((i, *order[q])):
                    axis = (rot + leg) % 3
                    at[axis] = upstream(axis, -sign if theirs else sign, hop)
                wsm[slot * 6 + p] = w_ref[0, device(at, 1 - core if theirs else core)]

    lane = lax.broadcasted_iota(jnp.int32, (1, 128), 1)
    lane_full = lax.broadcasted_iota(jnp.int32, (ROWS, 128), 1)

    def prepare(slot, buf, place):
        x = xb[slot, :, 0:384].astype(F32)
        sq = x * x
        nx = jnp.sum(sq[:, 0:128] + sq[:, 128:256] + sq[:, 256:384], axis=1, keepdims=True)
        hi, mid, low = split3(-0.5 * nx)
        cols = jnp.where(lane_full < 3, 1.0, 0.0)
        cols = jnp.where(lane_full == 3, hi, cols)
        cols = jnp.where(lane_full == 4, mid, cols)
        cols = jnp.where(lane_full == 5, low, cols)
        base = pl.multiple_of(place * ROWS, ROWS)
        aug[buf][pl.ds(base, ROWS), :] = cols.astype(BF16)
        w = wsm[slot * 6 + 5]
        for p in range(4, -1, -1):
            w = jnp.where(lane < PIECES[p + 1][0], wsm[slot * 6 + p], w)
        v_t = xb[slot, :, 384:512].T[0:64, :]
        stage[:, pl.ds(base, ROWS)] = (v_t.astype(F32) * w.astype(F32)).astype(BF16)

    send_own()
    mask_words(0, False)

    vt[...] = jnp.zeros_like(vt)
    stage[...] = jnp.zeros_like(stage)
    ks0[...] = jnp.zeros_like(ks0)
    ks1[...] = jnp.zeros_like(ks1)
    y_ref[...] = jnp.zeros_like(y_ref)
    z_in.wait()
    row = lax.broadcasted_iota(jnp.int32, (128, tile), 0)

    def prepare_targets(r, carry):
        base = pl.multiple_of(r * tile, tile)
        zr = zv[pl.ds(base, tile), :].T
        zt[0:384, pl.ds(base, tile)] = zr
        zf = zr.astype(F32)
        hi, mid, low = split3(-0.5 * jnp.sum(zf * zf, axis=0, keepdims=True))
        rows = jnp.where(row == 0, hi, jnp.where(row == 1, mid, jnp.where(row == 2, low, 0.0)))
        rows = jnp.where((row >= 3) & (row < 6), 1.0, rows)
        zt[384:512, pl.ds(base, tile)] = rows.astype(BF16)
        return carry

    lax.fori_loop(0, TILES, prepare_targets, 0)
    ell = jnp.full((1, tile), ell_ref[0], F32)
    rate = LOG2E / (ell * ell)
    scale = scale_ref[0]

    prepare(0, 0, 0)
    arrive(0)
    forward(0)
    to_partner(0)
    for n in range(1, ring):
        prepare(n, 0, n)

    def product(buf, ks, at):
        base = pl.multiple_of(at * tile, tile)
        y_ref[:, pl.ds(base, tile)] += jnp.dot(vt[buf], ks[...], preferred_element_type=F32)

    def run_chunk(g, prep):
        first = 2 * ring * g + (ring if g == n_groups else 0)
        count = ring if g in (0, n_groups) else 2 * ring
        rows = count * ROWS
        vt[g % 2] = stage[...]
        if g == n_groups - 1:
            stage[:, half:] = jnp.zeros((64, half), BF16)

        def block(r, ks):
            src = xb[pl.ds(first, count)].reshape(rows, 512)[:, 0:384]
            lhs = jnp.concatenate([src, aug[g % 2][0:rows, :]], axis=1)
            base = pl.multiple_of(r * tile, tile)
            neg = jnp.dot(lhs, zt[:, pl.ds(base, tile)], preferred_element_type=F32)
            val = jnp.exp2(jnp.minimum(neg * rate, 0.0)) * scale
            ks[0:rows, :] = val.astype(BF16)

        def body(m, carry):
            product(jnp.where(m == 0, (g + 1) % 2, g % 2), ks1, (2 * m + TILES - 1) % TILES)
            block(2 * m, ks0)
            if prep:
                prepare_next(g + 1, m)
            block(2 * m + 1, ks1)
            product(g % 2, ks0, 2 * m)
            return carry

        lax.fori_loop(0, TILES // 2, body, 0)

    def prepare_next(n, m):
        for u in range(per_body):
            place = m * per_body + u
            if n < n_groups:
                prepare(2 * ring * n + place, n % 2, place)
            if n >= 1:
                prepare(2 * ring * n + ring + place, n % 2, place + (0 if n == n_groups else ring))

    def communicate(n):
        if n < n_groups:
            arrive(n)
            forward(n)
            to_partner(n)
            mask_words(n, False)
        mask_words(n - 1, True)
        from_partner(n - 1)

    for g in range(n_groups + 1):
        if g == n_groups:
            run_chunk(g, False)
        elif g < EARLY:
            run_chunk(g, False)
            communicate(g + 1)

            def prep_body(m, carry, n=g + 1):
                prepare_next(n, m)
                return carry

            lax.fori_loop(0, TILES // 2, prep_body, 0)
        else:
            communicate(g + 1)
            run_chunk(g, True)
    product(n_groups % 2, ks1, TILES - 1)
    for q in range(n_groups):
        done = xb.at[pl.ds(0, sent[q])]
        pltpu.make_async_copy(done, done, send_sem.at[q]).wait()


def solution(mesh):
    devices = mesh.shape["sp"]
    ring = round((devices // 2) ** (1 / 3))
    n_groups = ring**2
    slots = 2 * ring * (n_groups + 1)
    rows = 2 * ring * ROWS
    row_spec = P(("dp", "sp"), None)

    def local_fn(z_rows, x_rows, v_rows, mask_row, length_scale, out_scale):
        targets = z_rows.shape[0]
        tile = targets // TILES
        pad = jnp.zeros((ROWS, 128 - v_rows.shape[1]), BF16)
        packed = jnp.concatenate([x_rows, v_rows, pad], axis=1)
        y_t = pl.pallas_call(
            functools.partial(kernel, ring),
            out_shape=jax.ShapeDtypeStruct((64, targets), F32),
            in_specs=[
                pl.BlockSpec(memory_space=pl.ANY),
                pl.BlockSpec(memory_space=pl.ANY),
                pl.BlockSpec(memory_space=pltpu.SMEM),
                pl.BlockSpec(memory_space=pltpu.SMEM),
                pl.BlockSpec(memory_space=pltpu.SMEM),
            ],
            out_specs=pl.BlockSpec(memory_space=pltpu.VMEM),
            scratch_shapes=[
                pltpu.VMEM((slots, ROWS, 512), BF16),
                pltpu.VMEM((targets, 384), BF16),
                pltpu.VMEM((512, targets), BF16),
                pltpu.VMEM((rows, 128), BF16),
                pltpu.VMEM((rows, 128), BF16),
                pltpu.VMEM((64, rows), BF16),
                pltpu.VMEM((2, 64, rows), BF16),
                pltpu.VMEM((rows, tile), BF16),
                pltpu.VMEM((rows, tile), BF16),
                pltpu.SMEM((slots * 6,), jnp.int32),
                pltpu.SemaphoreType.DMA((2,)),
                pltpu.SemaphoreType.DMA((n_groups,)),
                pltpu.SemaphoreType.DMA((n_groups,)),
                pltpu.SemaphoreType.DMA((n_groups,)),
            ],
            compiler_params=pltpu.CompilerParams(
                collective_id=0, has_side_effects=True, vmem_limit_bytes=60 * 2**20
            ),
            name="gather_product",
        )(packed, z_rows, mask_row, length_scale, out_scale)
        return y_t.T

    return jax.shard_map(
        local_fn,
        mesh=mesh,
        in_specs=(row_spec, row_spec, row_spec, row_spec, P(None), P(None)),
        out_specs=row_spec,
        check_vma=False,
    )
```

```python
import functools

import jax
import jax.numpy as jnp
from jax import lax
from jax.experimental import pallas as pl
from jax.experimental.pallas import tpu as pltpu
from jax.sharding import PartitionSpec as P

MESH = pl.DeviceIdType.MESH
F32 = jnp.float32
BF16 = jnp.bfloat16
LOG2E = 1.4426950408889634
ROWS = 128
PIECES = ((0, 32, 0, 1), (32, 16, 0, -1), (48, 32, 1, 1), (80, 16, 1, -1), (96, 16, 2, 1), (112, 16, 2, -1))
TILES = 2
PART = 2


def line_order(ring):
    hops = [(j, k) for j in range(ring) for k in range(ring)]
    return sorted(hops, key=lambda h: (sum(h), h[1], h[0]))


def split3(val):
    hi = val.astype(BF16).astype(F32)
    rest = val - hi
    mid = rest.astype(BF16).astype(F32)
    return hi, mid, (rest - mid).astype(BF16).astype(F32)


def kernel(ring, x_hbm, z_hbm, w_ref, ell_ref, scale_ref, y_ref,
           xb, zv, zt, aug, aug_next, stage, vt, ks0, ks1, wsm, in_sem, recv_sem, pair_sem, send_sem):
    order = line_order(ring)
    slot_of = {h: n for n, h in enumerate(order)}
    n_groups = len(order)
    half = ring * ROWS
    tile = zv.shape[0] // TILES

    me = lax.axis_index("sp")
    core = me % 2
    pos = [(me // 2) % ring, (me // (2 * ring)) % ring, me // (2 * ring * ring)]
    step = 1 - 2 * core
    shifted = [[(p + (ring - h) * step + ring * ring) % ring for h in range(ring)] for p in pos]

    def device(coords, c):
        x, y, z = coords
        return ((z * ring + y) * ring + x) * 2 + c

    def upstream(axis, sign, hop):
        return shifted[axis][hop if sign > 0 else (ring - hop) % ring]

    def downstream(axis, sign, hop):
        at = list(pos)
        at[axis] = upstream(axis, sign, (ring - hop) % ring)
        return device(at, core)

    partner = me + step

    own_in = pltpu.make_async_copy(x_hbm, xb.at[0], in_sem.at[0])
    z_in = pltpu.make_async_copy(z_hbm, zv, in_sem.at[1])
    own_in.start()
    z_in.start()
    barrier = pltpu.get_barrier_semaphore()
    others = [downstream(axis, 1, hop) for axis in range(3) for hop in range(1, ring)] + [partner]
    for other in others:
        pl.semaphore_signal(barrier, inc=1, device_id={"sp": other}, device_id_type=MESH)
    pl.semaphore_wait(barrier, len(others))
    own_in.wait()

    sent = [0] * n_groups

    def send(src, dst, axis, sign, hop, q, m):
        pltpu.make_async_remote_copy(
            src_ref=src,
            dst_ref=dst,
            send_sem=send_sem.at[q],
            recv_sem=recv_sem.at[m],
            device_id={"sp": downstream(axis, sign, hop)},
            device_id_type=MESH,
        ).start()

    def send_own():
        for hop in sorted(range(1, ring), key=lambda h: min(h, ring - h)):
            for lo, cnt, rot, sign in PIECES:
                rows = pl.ds(lo, cnt)
                send(xb.at[0, rows], xb.at[hop, rows], rot, sign, hop, 0, 0)
            sent[0] += 1

    def forward(q):
        j, k = order[q]
        for leg, child in ((1, (j + 1, k) if k == 0 else None), (2, (j, k + 1))):
            if child not in slot_of:
                continue
            m = slot_of[child]
            for lo, cnt, rot, sign in PIECES:
                rows = pl.ds(lo, cnt)
                send(
                    xb.at[pl.ds(2 * ring * q, ring), rows],
                    xb.at[pl.ds(2 * ring * m, ring), rows],
                    (rot + leg) % 3, sign, 1, q, m,
                )
            sent[q] += ring

    def arrive(q):
        dst = xb.at[pl.ds(1, ring - 1)] if q == 0 else xb.at[pl.ds(2 * ring * q, ring)]
        pltpu.make_async_copy(dst, dst, recv_sem.at[q]).wait()

    def to_partner(q):
        pltpu.make_async_remote_copy(
            src_ref=xb.at[pl.ds(2 * ring * q, ring)],
            dst_ref=xb.at[pl.ds(2 * ring * (q + 1) + ring, ring)],
            send_sem=send_sem.at[q],
            recv_sem=pair_sem.at[q],
            device_id={"sp": partner},
            device_id_type=MESH,
        ).start()
        sent[q] += ring

    def from_partner(q):
        dst = xb.at[pl.ds(2 * ring * (q + 1) + ring, ring)]
        pltpu.make_async_copy(dst, dst, pair_sem.at[q]).wait()

    def mask_words(q, theirs):
        for i in range(ring):
            slot = (2 * ring * (q + 1) + ring if theirs else 2 * ring * q) + i
            for p, (_, _, rot, sign) in enumerate(PIECES):
                at = [None] * 3
                for leg, hop in enumerate((i, *order[q])):
                    axis = (rot + leg) % 3
                    at[axis] = upstream(axis, -sign if theirs else sign, hop)
                wsm[slot * 6 + p] = w_ref[0, device(at, 1 - core if theirs else core)]

    lane = lax.broadcasted_iota(jnp.int32, (1, 128), 1)
    lane_full = lax.broadcasted_iota(jnp.int32, (ROWS, 128), 1)

    def prepare(slot, place):
        x = xb[slot, :, 0:384].astype(F32)
        sq = x * x
        nx = jnp.sum(sq[:, 0:128] + sq[:, 128:256] + sq[:, 256:384], axis=1, keepdims=True)
        hi, mid, low = split3(-0.5 * nx)
        cols = jnp.where(lane_full < 3, 1.0, 0.0)
        cols = jnp.where(lane_full == 3, hi, cols)
        cols = jnp.where(lane_full == 4, mid, cols)
        cols = jnp.where(lane_full == 5, low, cols)
        at = pl.ds(place * ROWS, ROWS)
        aug_next[at, :] = cols.astype(BF16)
        w = wsm[slot * 6 + 5]
        for p in range(4, -1, -1):
            w = jnp.where(lane < PIECES[p + 1][0], wsm[slot * 6 + p], w)
        v_t = xb[slot, :, 384:512].T[0:64, :]
        stage[:, at] = (v_t.astype(F32) * w.astype(F32)).astype(BF16)

    send_own()
    mask_words(0, False)

    vt[...] = jnp.zeros_like(vt)
    stage[...] = jnp.zeros_like(stage)
    ks0[...] = jnp.zeros_like(ks0)
    ks1[...] = jnp.zeros_like(ks1)
    y_ref[...] = jnp.zeros_like(y_ref)
    z_in.wait()
    narrow = tile // 2
    row = lax.broadcasted_iota(jnp.int32, (128, narrow), 0)

    def prepare_targets(r, carry):
        base = pl.multiple_of(r * narrow, narrow)
        zr = zv[pl.ds(base, narrow), :].T
        zt[0:384, pl.ds(base, narrow)] = zr
        zf = zr.astype(F32)
        hi, mid, low = split3(-0.5 * jnp.sum(zf * zf, axis=0, keepdims=True))
        rows = jnp.where(row == 0, hi, jnp.where(row == 1, mid, jnp.where(row == 2, low, 0.0)))
        rows = jnp.where((row >= 3) & (row < 6), 1.0, rows)
        zt[384:512, pl.ds(base, narrow)] = rows.astype(BF16)
        return carry

    lax.fori_loop(0, 2 * TILES, prepare_targets, 0)
    ell = jnp.full((1, 1), ell_ref[0], F32)
    rate = LOG2E / (ell * ell)
    scale = scale_ref[0]

    prepare(0, 0)
    arrive(0)
    forward(0)
    to_partner(0)
    for n in range(1, ring):
        prepare(n, n)
    tiles = (ks0, ks1)

    def product(buf, u, part):
        rows = slice(part * PART * ROWS, (part + 1) * PART * ROWS)
        cols = slice(u * tile, (u + 1) * tile)
        y_ref[:, cols] += jnp.dot(vt[buf, :, rows], tiles[u][rows, :], preferred_element_type=F32)

    def block(first, u, part):
        rows = slice(part * PART * ROWS, (part + 1) * PART * ROWS)
        src = xb[pl.ds(first + part * PART, PART)].reshape(PART * ROWS, 512)[:, 0:384]
        lhs = jnp.concatenate([src, aug[rows, :]], axis=1)
        neg = jnp.dot(lhs, zt[:, u * tile:(u + 1) * tile], preferred_element_type=F32)
        val = jnp.exp2(jnp.minimum(neg * rate, 0.0)) * scale
        tiles[u][rows, :] = val.astype(BF16)

    def run_chunk(g, parts, prep):
        first = 2 * ring * g
        vt[g % 2] = stage[...]
        aug[...] = aug_next[...]
        for u in range(TILES):
            for part in range(ring):
                if part in parts:
                    block(first, u, part)
                product((g + 1) % 2 if u == 0 else g % 2, (u + TILES - 1) % TILES, part)
                if prep:
                    place = u * ring + part
                    prepare(2 * ring * (g + 1) + place, place)

    def communicate(n):
        if n < n_groups:
            arrive(n)
            forward(n)
            to_partner(n)
            mask_words(n, False)
        mask_words(n - 1, True)
        from_partner(n - 1)

    run_chunk(0, range(ring // PART), False)
    communicate(1)
    for place in range(2 * ring):
        prepare(2 * ring + place, place)

    def chunk(g, carry):
        for low in range(1, n_groups, ring):
            high = min(low + ring, n_groups)

            @pl.when((g >= low) & (g < high))
            def _(low=low, high=high):
                for n in range(low, high):

                    @pl.when(g == n)
                    def _(n=n):
                        communicate(n + 1)

        run_chunk(g, range(ring), True)
        return carry

    lax.fori_loop(1, n_groups, chunk, 0)
    stage[:, 0:half] = jnp.zeros((64, half), BF16)
    run_chunk(n_groups, range(ring // PART, ring), False)
    for part in range(ring):
        product(n_groups % 2, TILES - 1, part)
    for q in range(n_groups):
        done = xb.at[pl.ds(0, sent[q])]
        pltpu.make_async_copy(done, done, send_sem.at[q]).wait()


def solution(mesh):
    devices = mesh.shape["sp"]
    ring = round((devices // 2) ** (1 / 3))
    n_groups = ring**2
    slots = 2 * ring * (n_groups + 1)
    rows = 2 * ring * ROWS
    row_spec = P(("dp", "sp"), None)

    def local_fn(z_rows, x_rows, v_rows, mask_row, length_scale, out_scale):
        targets = z_rows.shape[0]
        tile = targets // TILES
        pad = jnp.zeros((ROWS, 128 - v_rows.shape[1]), BF16)
        packed = jnp.concatenate([x_rows, v_rows, pad], axis=1)
        y_t = pl.pallas_call(
            functools.partial(kernel, ring),
            out_shape=jax.ShapeDtypeStruct((64, targets), F32),
            in_specs=[
                pl.BlockSpec(memory_space=pl.ANY),
                pl.BlockSpec(memory_space=pl.ANY),
                pl.BlockSpec(memory_space=pltpu.SMEM),
                pl.BlockSpec(memory_space=pltpu.SMEM),
                pl.BlockSpec(memory_space=pltpu.SMEM),
            ],
            out_specs=pl.BlockSpec(memory_space=pltpu.VMEM),
            scratch_shapes=[
                pltpu.VMEM((slots, ROWS, 512), BF16),
                pltpu.VMEM((targets, 384), BF16),
                pltpu.VMEM((512, targets), BF16),
                pltpu.VMEM((rows, 128), BF16),
                pltpu.VMEM((rows, 128), BF16),
                pltpu.VMEM((64, rows), BF16),
                pltpu.VMEM((2, 64, rows), BF16),
                pltpu.VMEM((rows, tile), BF16),
                pltpu.VMEM((rows, tile), BF16),
                pltpu.SMEM((slots * 6,), jnp.int32),
                pltpu.SemaphoreType.DMA((2,)),
                pltpu.SemaphoreType.DMA((n_groups,)),
                pltpu.SemaphoreType.DMA((n_groups,)),
                pltpu.SemaphoreType.DMA((n_groups,)),
            ],
            compiler_params=pltpu.CompilerParams(
                collective_id=0, has_side_effects=True, vmem_limit_bytes=60 * 2**20
            ),
            name="gather_product",
        )(packed, z_rows, mask_row, length_scale, out_scale)
        return y_t.T

    return jax.shard_map(
        local_fn,
        mesh=mesh,
        in_specs=(row_spec, row_spec, row_spec, row_spec, P(None), P(None)),
        out_specs=row_spec,
        check_vma=False,
    )
```

```python
import functools

import jax
import jax.numpy as jnp
from jax import lax
from jax.experimental import pallas as pl
from jax.experimental.pallas import tpu as pltpu
from jax.sharding import PartitionSpec as P

MESH = pl.DeviceIdType.MESH
F32 = jnp.float32
BF16 = jnp.bfloat16
LOG2E = 1.4426950408889634
ROWS = 128
PIECES = ((0, 32, 0, 1), (32, 16, 0, -1), (48, 32, 1, 1), (80, 16, 1, -1), (96, 16, 2, 1), (112, 16, 2, -1))
TILES = 2
PART = 2


def line_order(ring):
    hops = [(j, k) for j in range(ring) for k in range(ring)]
    return sorted(hops, key=lambda h: (sum(h), h[1], h[0]))


def split3(val):
    hi = val.astype(BF16).astype(F32)
    rest = val - hi
    mid = rest.astype(BF16).astype(F32)
    return hi, mid, (rest - mid).astype(BF16).astype(F32)


def kernel(ring, x_hbm, v_hbm, z_hbm, w_ref, ell_ref, scale_ref, y_ref,
           xb, zv, zt, vin, aug, aug_next, stage, vt, ks0, ks1, wsm, in_sem, line_sem, recv_sem, pair_sem, send_sem):
    order = line_order(ring)
    slot_of = {h: n for n, h in enumerate(order)}
    n_groups = len(order)
    half = ring * ROWS
    tile = zv.shape[0] // TILES

    me = lax.axis_index("sp")
    core = me % 2
    pos = [(me // 2) % ring, (me // (2 * ring)) % ring, me // (2 * ring * ring)]
    step = 1 - 2 * core
    shifted = [[(p + (ring - h) * step + ring * ring) % ring for h in range(ring)] for p in pos]

    def device(coords, c):
        x, y, z = coords
        return ((z * ring + y) * ring + x) * 2 + c

    def upstream(axis, sign, hop):
        return shifted[axis][hop if sign > 0 else (ring - hop) % ring]

    def downstream(axis, sign, hop):
        at = list(pos)
        at[axis] = upstream(axis, sign, (ring - hop) % ring)
        return device(at, core)

    partner = me + step

    own_in = pltpu.make_async_copy(x_hbm, xb.at[0, :, pl.ds(0, 384)], in_sem.at[0])
    v_in = pltpu.make_async_copy(v_hbm, vin, in_sem.at[2])
    z_in = pltpu.make_async_copy(z_hbm, zv, in_sem.at[1])
    v_in.start()
    own_in.start()
    z_in.start()
    barrier = pltpu.get_barrier_semaphore()
    others = [downstream(axis, 1, hop) for axis in range(3) for hop in range(1, ring)] + [partner]
    for other in others:
        pl.semaphore_signal(barrier, inc=1, device_id={"sp": other}, device_id_type=MESH)
    v_in.wait()
    xb[0, :, 384:512] = jnp.concatenate([vin[...], jnp.zeros_like(vin)], axis=0).T
    pl.semaphore_wait(barrier, len(others))
    own_in.wait()

    sent = [0] * n_groups
    nearest = sorted(range(1, ring), key=lambda h: min(h, ring - h))

    def send(src, dst, axis, sign, hop, q, landed):
        pltpu.make_async_remote_copy(
            src_ref=src,
            dst_ref=dst,
            send_sem=send_sem.at[q],
            recv_sem=landed,
            device_id={"sp": downstream(axis, sign, hop)},
            device_id_type=MESH,
        ).start()

    def send_own():
        for hop in nearest:
            for lo, cnt, rot, sign in PIECES:
                rows = pl.ds(lo, cnt)
                send(xb.at[0, rows], xb.at[hop, rows], rot, sign, hop, 0, line_sem.at[hop])
            sent[0] += 1

    def forward(q, i=None):
        here, count = (0, ring) if i is None else (i, 1)
        j, k = order[q]
        for leg, child in ((1, (j + 1, k) if k == 0 else None), (2, (j, k + 1))):
            if child not in slot_of:
                continue
            m = slot_of[child]
            for lo, cnt, rot, sign in PIECES:
                rows = pl.ds(lo, cnt)
                send(
                    xb.at[pl.ds(2 * ring * q + here, count), rows],
                    xb.at[pl.ds(2 * ring * m + here, count), rows],
                    (rot + leg) % 3, sign, 1, q, recv_sem.at[m],
                )
            sent[q] += count

    def arrive(q):
        dst = xb.at[pl.ds(2 * ring * q, ring)]
        pltpu.make_async_copy(dst, dst, recv_sem.at[q]).wait()

    def to_partner(q):
        pltpu.make_async_remote_copy(
            src_ref=xb.at[pl.ds(2 * ring * q, ring)],
            dst_ref=xb.at[pl.ds(2 * ring * (q + 1) + ring, ring)],
            send_sem=send_sem.at[q],
            recv_sem=pair_sem.at[q],
            device_id={"sp": partner},
            device_id_type=MESH,
        ).start()
        sent[q] += ring

    def from_partner(q):
        dst = xb.at[pl.ds(2 * ring * (q + 1) + ring, ring)]
        pltpu.make_async_copy(dst, dst, pair_sem.at[q]).wait()

    def mask_words(q, theirs):
        for i in range(ring):
            slot = (2 * ring * (q + 1) + ring if theirs else 2 * ring * q) + i
            for p, (_, _, rot, sign) in enumerate(PIECES):
                at = [None] * 3
                for leg, hop in enumerate((i, *order[q])):
                    axis = (rot + leg) % 3
                    at[axis] = upstream(axis, -sign if theirs else sign, hop)
                wsm[slot * 6 + p] = w_ref[0, device(at, 1 - core if theirs else core)]

    lane = lax.broadcasted_iota(jnp.int32, (1, 128), 1)
    lane_full = lax.broadcasted_iota(jnp.int32, (ROWS, 128), 1)

    def prepare(slot, place):
        x = xb[slot, :, 0:384].astype(F32)
        sq = x * x
        nx = jnp.sum(sq[:, 0:128] + sq[:, 128:256] + sq[:, 256:384], axis=1, keepdims=True)
        hi, mid, low = split3(-0.5 * nx)
        cols = jnp.where(lane_full < 3, 1.0, 0.0)
        cols = jnp.where(lane_full == 3, hi, cols)
        cols = jnp.where(lane_full == 4, mid, cols)
        cols = jnp.where(lane_full == 5, low, cols)
        at = pl.ds(place * ROWS, ROWS)
        aug_next[at, :] = cols.astype(BF16)
        w = wsm[slot * 6 + 5]
        for p in range(4, -1, -1):
            w = jnp.where(lane < PIECES[p + 1][0], wsm[slot * 6 + p], w)
        v_t = xb[slot, :, 384:512].T[0:64, :]
        stage[:, at] = (v_t.astype(F32) * w.astype(F32)).astype(BF16)

    send_own()
    forward(0, 0)
    mask_words(0, False)

    vt[...] = jnp.zeros_like(vt)
    stage[...] = jnp.zeros_like(stage)
    ks0[...] = jnp.zeros_like(ks0)
    ks1[...] = jnp.zeros_like(ks1)
    y_ref[...] = jnp.zeros_like(y_ref)
    z_in.wait()
    narrow = tile // 2
    row = lax.broadcasted_iota(jnp.int32, (128, narrow), 0)

    def prepare_targets(r, carry):
        base = pl.multiple_of(r * narrow, narrow)
        zr = zv[pl.ds(base, narrow), :].T
        zt[0:384, pl.ds(base, narrow)] = zr
        zf = zr.astype(F32)
        hi, mid, low = split3(-0.5 * jnp.sum(zf * zf, axis=0, keepdims=True))
        rows = jnp.where(row == 0, hi, jnp.where(row == 1, mid, jnp.where(row == 2, low, 0.0)))
        rows = jnp.where((row >= 3) & (row < 6), 1.0, rows)
        zt[384:512, pl.ds(base, narrow)] = rows.astype(BF16)
        return carry

    lax.fori_loop(0, 2 * TILES, prepare_targets, 0)
    ell = jnp.full((1, 1), ell_ref[0], F32)
    rate = LOG2E / (ell * ell)
    scale = scale_ref[0]

    prepare(0, 0)
    for hop in nearest:
        dst = xb.at[hop]
        pltpu.make_async_copy(dst, dst, line_sem.at[hop]).wait()
        forward(0, hop)
    to_partner(0)
    for n in range(1, ring):
        prepare(n, n)
    tiles = (ks0, ks1)

    def product(buf, u, part):
        rows = slice(part * PART * ROWS, (part + 1) * PART * ROWS)
        cols = slice(u * tile, (u + 1) * tile)
        y_ref[:, cols] += jnp.dot(vt[buf, :, rows], tiles[u][rows, :], preferred_element_type=F32)

    def block(first, u, part):
        rows = slice(part * PART * ROWS, (part + 1) * PART * ROWS)
        src = xb[pl.ds(first + part * PART, PART)].reshape(PART * ROWS, 512)[:, 0:384]
        lhs = jnp.concatenate([src, aug[rows, :]], axis=1)
        neg = jnp.dot(lhs, zt[:, u * tile:(u + 1) * tile], preferred_element_type=F32)
        val = jnp.exp2(jnp.minimum(neg * rate, 0.0)) * scale
        tiles[u][rows, :] = val.astype(BF16)

    def run_chunk(g, parts, prep):
        first = 2 * ring * g
        vt[g % 2] = stage[...]
        aug[...] = aug_next[...]
        for u in range(TILES):
            for part in range(ring):
                if part in parts:
                    block(first, u, part)
                product((g + 1) % 2 if u == 0 else g % 2, (u + TILES - 1) % TILES, part)
                if prep:
                    place = u * ring + part
                    prepare(2 * ring * (g + 1) + place, place)

    def communicate(n):
        if n < n_groups:
            arrive(n)
            forward(n)
            to_partner(n)
            mask_words(n, False)
        mask_words(n - 1, True)
        from_partner(n - 1)

    run_chunk(0, range(ring // PART), False)
    communicate(1)
    for place in range(2 * ring):
        prepare(2 * ring + place, place)

    def chunk(g, carry):
        for low in range(1, n_groups, ring):
            high = min(low + ring, n_groups)

            @pl.when((g >= low) & (g < high))
            def _(low=low, high=high):
                for n in range(low, high):

                    @pl.when(g == n)
                    def _(n=n):
                        communicate(n + 1)

        run_chunk(g, range(ring), True)
        return carry

    lax.fori_loop(1, n_groups, chunk, 0)
    stage[:, 0:half] = jnp.zeros((64, half), BF16)
    run_chunk(n_groups, range(ring // PART, ring), False)
    for part in range(ring):
        product(n_groups % 2, TILES - 1, part)
    for q in range(n_groups):
        done = xb.at[pl.ds(0, sent[q])]
        pltpu.make_async_copy(done, done, send_sem.at[q]).wait()


def solution(mesh):
    devices = mesh.shape["sp"]
    ring = round((devices // 2) ** (1 / 3))
    n_groups = ring**2
    slots = 2 * ring * (n_groups + 1)
    rows = 2 * ring * ROWS
    row_spec = P(("dp", "sp"), None)

    def local_fn(z_rows, x_rows, v_rows, mask_row, length_scale, out_scale):
        targets = z_rows.shape[0]
        tile = targets // TILES
        y_t = pl.pallas_call(
            functools.partial(kernel, ring),
            out_shape=jax.ShapeDtypeStruct((64, targets), F32),
            in_specs=[
                pl.BlockSpec(memory_space=pl.ANY),
                pl.BlockSpec(memory_space=pl.ANY),
                pl.BlockSpec(memory_space=pl.ANY),
                pl.BlockSpec(memory_space=pltpu.SMEM),
                pl.BlockSpec(memory_space=pltpu.SMEM),
                pl.BlockSpec(memory_space=pltpu.SMEM),
            ],
            out_specs=pl.BlockSpec(memory_space=pltpu.VMEM),
            scratch_shapes=[
                pltpu.VMEM((slots, ROWS, 512), BF16),
                pltpu.VMEM((targets, 384), BF16),
                pltpu.VMEM((512, targets), BF16),
                pltpu.VMEM((64, ROWS), BF16),
                pltpu.VMEM((rows, 128), BF16),
                pltpu.VMEM((rows, 128), BF16),
                pltpu.VMEM((64, rows), BF16),
                pltpu.VMEM((2, 64, rows), BF16),
                pltpu.VMEM((rows, tile), BF16),
                pltpu.VMEM((rows, tile), BF16),
                pltpu.SMEM((slots * 6,), jnp.int32),
                pltpu.SemaphoreType.DMA((3,)),
                pltpu.SemaphoreType.DMA((ring,)),
                pltpu.SemaphoreType.DMA((n_groups,)),
                pltpu.SemaphoreType.DMA((n_groups,)),
                pltpu.SemaphoreType.DMA((n_groups,)),
            ],
            compiler_params=pltpu.CompilerParams(
                collective_id=0, has_side_effects=True, vmem_limit_bytes=60 * 2**20
            ),
            name="gather_product",
        )(x_rows, v_rows.T, z_rows, mask_row, length_scale, out_scale)
        return y_t.T

    return jax.shard_map(
        local_fn,
        mesh=mesh,
        in_specs=(row_spec, row_spec, row_spec, row_spec, P(None), P(None)),
        out_specs=row_spec,
        check_vma=False,
    )
```

```python
import functools

import jax
import jax.numpy as jnp
from jax import lax
from jax.experimental import pallas as pl
from jax.experimental.pallas import tpu as pltpu
from jax.sharding import PartitionSpec as P

MESH = pl.DeviceIdType.MESH
F32 = jnp.float32
BF16 = jnp.bfloat16
LOG2E = 1.4426950408889634
ROWS = 128
PIECES = ((0, 32, 0, 1), (32, 16, 0, -1), (48, 32, 1, 1), (80, 16, 1, -1), (96, 16, 2, 1), (112, 16, 2, -1))
TILES = 2
PART = 2


def line_order(ring):
    hops = [(j, k) for j in range(ring) for k in range(ring)]
    return sorted(hops, key=lambda h: (sum(h), h[1], h[0]))


def split3(val):
    hi = val.astype(BF16).astype(F32)
    rest = val - hi
    mid = rest.astype(BF16).astype(F32)
    return hi, mid, (rest - mid).astype(BF16).astype(F32)


def kernel(ring, x_hbm, v_hbm, z_hbm, w_ref, ell_ref, scale_ref, y_ref,
           xb, zv, zt, vin, aug0, aug1, stage, vt, ks0, ks1, wsm, in_sem, line_sem, recv_sem, pair_sem, send_sem):
    order = line_order(ring)
    slot_of = {h: n for n, h in enumerate(order)}
    n_groups = len(order)
    half = ring * ROWS
    tile = zv.shape[0] // TILES

    me = lax.axis_index("sp")
    core = me % 2
    pos = [(me // 2) % ring, (me // (2 * ring)) % ring, me // (2 * ring * ring)]
    step = 1 - 2 * core
    shifted = [[(p + (ring - h) * step + ring * ring) % ring for h in range(ring)] for p in pos]

    def device(coords, c):
        x, y, z = coords
        return ((z * ring + y) * ring + x) * 2 + c

    def upstream(axis, sign, hop):
        return shifted[axis][hop if sign > 0 else (ring - hop) % ring]

    def downstream(axis, sign, hop):
        at = list(pos)
        at[axis] = upstream(axis, sign, (ring - hop) % ring)
        return device(at, core)

    partner = me + step

    own_in = pltpu.make_async_copy(x_hbm, xb.at[0, :, pl.ds(0, 384)], in_sem.at[0])
    v_in = pltpu.make_async_copy(v_hbm, vin, in_sem.at[2])
    z_in = pltpu.make_async_copy(z_hbm, zv, in_sem.at[1])
    v_in.start()
    own_in.start()
    z_in.start()
    barrier = pltpu.get_barrier_semaphore()
    others = [downstream(axis, 1, hop) for axis in range(3) for hop in range(1, ring)] + [partner]
    for other in others:
        pl.semaphore_signal(barrier, inc=1, device_id={"sp": other}, device_id_type=MESH)
    v_in.wait()
    xb[0, :, 384:512] = jnp.concatenate([vin[...], jnp.zeros_like(vin)], axis=0).T
    pl.semaphore_wait(barrier, len(others))
    own_in.wait()

    sent = [0] * n_groups
    nearest = sorted(range(1, ring), key=lambda h: min(h, ring - h))

    def send(src, dst, axis, sign, hop, q, landed):
        pltpu.make_async_remote_copy(
            src_ref=src,
            dst_ref=dst,
            send_sem=send_sem.at[q],
            recv_sem=landed,
            device_id={"sp": downstream(axis, sign, hop)},
            device_id_type=MESH,
        ).start()

    def send_own():
        for hop in nearest:
            for lo, cnt, rot, sign in PIECES:
                rows = pl.ds(lo, cnt)
                send(xb.at[0, rows], xb.at[hop, rows], rot, sign, hop, 0, line_sem.at[hop])
            sent[0] += 1

    def forward(q, i=None):
        here, count = (0, ring) if i is None else (i, 1)
        j, k = order[q]
        for leg, child in ((1, (j + 1, k) if k == 0 else None), (2, (j, k + 1))):
            if child not in slot_of:
                continue
            m = slot_of[child]
            for lo, cnt, rot, sign in PIECES:
                rows = pl.ds(lo, cnt)
                send(
                    xb.at[pl.ds(2 * ring * q + here, count), rows],
                    xb.at[pl.ds(2 * ring * m + here, count), rows],
                    (rot + leg) % 3, sign, 1, q, recv_sem.at[m],
                )
            sent[q] += count

    def arrive(q):
        dst = xb.at[pl.ds(2 * ring * q, ring)]
        pltpu.make_async_copy(dst, dst, recv_sem.at[q]).wait()

    def to_partner(q):
        pltpu.make_async_remote_copy(
            src_ref=xb.at[pl.ds(2 * ring * q, ring)],
            dst_ref=xb.at[pl.ds(2 * ring * (q + 1) + ring, ring)],
            send_sem=send_sem.at[q],
            recv_sem=pair_sem.at[q],
            device_id={"sp": partner},
            device_id_type=MESH,
        ).start()
        sent[q] += ring

    def from_partner(q):
        dst = xb.at[pl.ds(2 * ring * (q + 1) + ring, ring)]
        pltpu.make_async_copy(dst, dst, pair_sem.at[q]).wait()

    def mask_words(q, theirs):
        for i in range(ring):
            slot = (2 * ring * (q + 1) + ring if theirs else 2 * ring * q) + i
            for p, (_, _, rot, sign) in enumerate(PIECES):
                at = [None] * 3
                for leg, hop in enumerate((i, *order[q])):
                    axis = (rot + leg) % 3
                    at[axis] = upstream(axis, -sign if theirs else sign, hop)
                wsm[slot * 6 + p] = w_ref[0, device(at, 1 - core if theirs else core)]

    lane = lax.broadcasted_iota(jnp.int32, (1, 128), 1)
    lane_full = lax.broadcasted_iota(jnp.int32, (ROWS, 128), 1)

    aug = (aug0, aug1)

    def prepare(slot, place, parity):
        x = xb[slot, :, 0:384].astype(F32)
        sq = x * x
        nx = jnp.sum(sq[:, 0:128] + sq[:, 128:256] + sq[:, 256:384], axis=1, keepdims=True)
        hi, mid, low = split3(-0.5 * nx)
        cols = jnp.where(lane_full < 3, 1.0, 0.0)
        cols = jnp.where(lane_full == 3, hi, cols)
        cols = jnp.where(lane_full == 4, mid, cols)
        cols = jnp.where(lane_full == 5, low, cols)
        at = pl.ds(place * ROWS, ROWS)
        aug[parity][at, :] = cols.astype(BF16)
        w = wsm[slot * 6 + 5]
        for p in range(4, -1, -1):
            w = jnp.where(lane < PIECES[p + 1][0], wsm[slot * 6 + p], w)
        v_t = xb[slot, :, 384:512].T[0:64, :]
        stage[:, at] = (v_t.astype(F32) * w.astype(F32)).astype(BF16)

    send_own()
    forward(0, 0)
    mask_words(0, False)

    vt[...] = jnp.zeros_like(vt)
    stage[...] = jnp.zeros_like(stage)
    ks0[...] = jnp.zeros_like(ks0)
    ks1[...] = jnp.zeros_like(ks1)
    y_ref[...] = jnp.zeros_like(y_ref)
    z_in.wait()
    narrow = tile // 2
    row = lax.broadcasted_iota(jnp.int32, (128, narrow), 0)

    def prepare_targets(r, carry):
        base = pl.multiple_of(r * narrow, narrow)
        zr = zv[pl.ds(base, narrow), :].T
        zt[0:384, pl.ds(base, narrow)] = zr
        zf = zr.astype(F32)
        hi, mid, low = split3(-0.5 * jnp.sum(zf * zf, axis=0, keepdims=True))
        rows = jnp.where(row == 0, hi, jnp.where(row == 1, mid, jnp.where(row == 2, low, 0.0)))
        rows = jnp.where((row >= 3) & (row < 6), 1.0, rows)
        zt[384:512, pl.ds(base, narrow)] = rows.astype(BF16)
        return carry

    lax.fori_loop(0, 2 * TILES, prepare_targets, 0)
    ell = jnp.full((1, 1), ell_ref[0], F32)
    rate = LOG2E / (ell * ell)
    scale = scale_ref[0]

    prepare(0, 0, 0)
    for hop in nearest:
        dst = xb.at[hop]
        pltpu.make_async_copy(dst, dst, line_sem.at[hop]).wait()
        forward(0, hop)
    to_partner(0)
    for n in range(1, ring):
        prepare(n, n, 0)
    tiles = (ks0, ks1)

    def product(buf, u, part):
        rows = slice(part * PART * ROWS, (part + 1) * PART * ROWS)
        cols = slice(u * tile, (u + 1) * tile)
        y_ref[:, cols] += jnp.dot(vt[buf, :, rows], tiles[u][rows, :], preferred_element_type=F32)

    def block(first, u, part, parity):
        rows = slice(part * PART * ROWS, (part + 1) * PART * ROWS)
        src = xb[pl.ds(first + part * PART, PART)].reshape(PART * ROWS, 512)[:, 0:384]
        lhs = jnp.concatenate([src, aug[parity][rows, :]], axis=1)
        neg = jnp.dot(lhs, zt[:, u * tile:(u + 1) * tile], preferred_element_type=F32)
        val = jnp.exp2(jnp.minimum(neg * rate, 0.0)) * scale
        tiles[u][rows, :] = val.astype(BF16)

    def run_chunk(g, parts, prep, parity):
        first = 2 * ring * g
        vt[parity] = stage[...]
        for u in range(TILES):
            for part in range(ring):
                if part in parts:
                    block(first, u, part, parity)
                product(1 - parity if u == 0 else parity, (u + TILES - 1) % TILES, part)
                if prep:
                    place = u * ring + part
                    prepare(2 * ring * (g + 1) + place, place, 1 - parity)

    def communicate(n):
        if n < n_groups:
            arrive(n)
            forward(n)
            to_partner(n)
            mask_words(n, False)
        mask_words(n - 1, True)
        from_partner(n - 1)

    run_chunk(0, range(ring // PART), False, 0)
    communicate(1)
    for place in range(2 * ring):
        prepare(2 * ring + place, place, 1)

    def chunk_pair(m, carry):
        for parity in (1, 0):
            g = 2 * m + 2 - parity
            for low in range(2 - parity, n_groups, 2 * ring):
                high = min(low + 2 * ring, n_groups)

                @pl.when((g >= low) & (g < high))
                def _(low=low, high=high, g=g):
                    for n in range(low, high, 2):
                        if n < n_groups - 1:

                            @pl.when(g == n)
                            def _(n=n):
                                communicate(n + 1)

            run_chunk(g, range(ring), True, parity)
        return carry

    lax.fori_loop(0, n_groups // 2 - 1, chunk_pair, 0)
    communicate(n_groups)
    run_chunk(n_groups - 1, range(ring), True, 1)
    stage[:, 0:half] = jnp.zeros((64, half), BF16)
    run_chunk(n_groups, range(ring // PART, ring), False, n_groups % 2)
    for part in range(ring):
        product(n_groups % 2, TILES - 1, part)
    for q in range(n_groups):
        done = xb.at[pl.ds(0, sent[q])]
        pltpu.make_async_copy(done, done, send_sem.at[q]).wait()


def solution(mesh):
    devices = mesh.shape["sp"]
    ring = round((devices // 2) ** (1 / 3))
    n_groups = ring**2
    slots = 2 * ring * (n_groups + 1)
    rows = 2 * ring * ROWS
    row_spec = P(("dp", "sp"), None)

    def local_fn(z_rows, x_rows, v_rows, mask_row, length_scale, out_scale):
        targets = z_rows.shape[0]
        tile = targets // TILES
        y_t = pl.pallas_call(
            functools.partial(kernel, ring),
            out_shape=jax.ShapeDtypeStruct((64, targets), F32),
            in_specs=[
                pl.BlockSpec(memory_space=pl.ANY),
                pl.BlockSpec(memory_space=pl.ANY),
                pl.BlockSpec(memory_space=pl.ANY),
                pl.BlockSpec(memory_space=pltpu.SMEM),
                pl.BlockSpec(memory_space=pltpu.SMEM),
                pl.BlockSpec(memory_space=pltpu.SMEM),
            ],
            out_specs=pl.BlockSpec(memory_space=pltpu.VMEM),
            scratch_shapes=[
                pltpu.VMEM((slots, ROWS, 512), BF16),
                pltpu.VMEM((targets, 384), BF16),
                pltpu.VMEM((512, targets), BF16),
                pltpu.VMEM((64, ROWS), BF16),
                pltpu.VMEM((rows, 128), BF16),
                pltpu.VMEM((rows, 128), BF16),
                pltpu.VMEM((64, rows), BF16),
                pltpu.VMEM((2, 64, rows), BF16),
                pltpu.VMEM((rows, tile), BF16),
                pltpu.VMEM((rows, tile), BF16),
                pltpu.SMEM((slots * 6,), jnp.int32),
                pltpu.SemaphoreType.DMA((3,)),
                pltpu.SemaphoreType.DMA((ring,)),
                pltpu.SemaphoreType.DMA((n_groups,)),
                pltpu.SemaphoreType.DMA((n_groups,)),
                pltpu.SemaphoreType.DMA((n_groups,)),
            ],
            compiler_params=pltpu.CompilerParams(
                collective_id=0, has_side_effects=True, vmem_limit_bytes=60 * 2**20
            ),
            name="gather_product",
        )(x_rows, v_rows.T, z_rows, mask_row, length_scale, out_scale)
        return y_t.T

    return jax.shard_map(
        local_fn,
        mesh=mesh,
        in_specs=(row_spec, row_spec, row_spec, row_spec, P(None), P(None)),
        out_specs=row_spec,
        check_vma=False,
    )
```
